32 devices in a mesh: groups: 2 (over y), seq: 8 (over z, x), vocab: 1, batch: 2 (over core).
Axes of the slice: x: 2, y: 2, z: 4, core: 2. Of those that a mesh axis runs over, the one named last changes fastest.
Arguments:
- queries: bfloat16 [4, 1536, 3584], P(('groups', 'vocab', 'batch'), 'seq'), parts along dimension 0, may hold values from -300 to 300
- keys: bfloat16 [4, 1536, 512], P(('groups', 'vocab', 'batch'), 'seq'), parts along dimension 0, may hold values from -10 to 10
- values: bfloat16 [4, 1536, 512], P(('groups', 'vocab', 'batch'), 'seq'), parts along dimension 0, may hold values from -24 to 24
- residual: bfloat16 [4, 1536, 3584], P(('groups', 'vocab', 'batch'), 'seq'), parts along dimension 0, may hold values from -2048 to 2048
- norm_gain: float32 [3584], replicated, may hold values from 0.5 to 1.5
Outputs:
- normed: bfloat16 [4, 1536, 3584], P(('groups', 'vocab', 'batch'), 'seq'), parts along dimension 0
The draws below stay inside these ranges and needn't reach their ends.
There are 2 independent parts, one for each index of `groups`. The reference program is written for one: setup_inputs(seed, part) draws one part's arguments, and reference() takes and returns one part's arrays. A program takes and returns all parts, laid end to end along the dimension named above; an argument that names none is the same for every part. Nothing has to cross between parts.
All inputs are finite; a program needn't handle non-finite values.
Results may differ from the reference program's by a relative error of at most 0.0049.
Values may be sent and summed in bfloat16 or wider, within the bound.
A program may use at most 128 MiB of HBM per device.

```python
import math
import jax
import jax.numpy as jnp
from jax import lax

D = 3584
QUERY_HEADS = 28
KEY_VALUE_HEADS = 4
HEAD_WIDTH = 128
RESPONSE_LENGTH = 1536
RESPONSE_COUNT = 2


def query_keys(key):
    key_start, key_query = jax.random.split(jax.random.fold_in(key, 11), 2)
    unscaled_keys = 1.5 * jax.random.truncated_normal(key_start, -6.0, 6.0, (RESPONSE_COUNT, RESPONSE_LENGTH, KEY_VALUE_HEADS, HEAD_WIDTH), jnp.float32)
    unscaled_query = 1.5 * jax.random.truncated_normal(key_query, -6.0, 6.0, (RESPONSE_COUNT, RESPONSE_LENGTH, QUERY_HEADS, HEAD_WIDTH), jnp.float32)
    return (unscaled_query.reshape(RESPONSE_COUNT, RESPONSE_LENGTH, QUERY_HEADS * HEAD_WIDTH), unscaled_keys.reshape(RESPONSE_COUNT, RESPONSE_LENGTH, KEY_VALUE_HEADS * HEAD_WIDTH))


def draw_queries(key, part):
    return query_keys(key)[0].astype(jnp.bfloat16)


def draw_keys(key, part):
    return query_keys(key)[1].astype(jnp.bfloat16)


def draw_residual(key, part):
    key_rows, key_columns, key_start = jax.random.split(jax.random.fold_in(key, 23), 3)
    row_scale = jnp.exp(jax.random.uniform(key_rows, (RESPONSE_COUNT, RESPONSE_LENGTH, 1), jnp.float32, math.log(0.3), math.log(3.0)))
    column_scale = jnp.exp(jax.random.uniform(key_columns, (1, 1, D), jnp.float32, math.log(0.3), math.log(3.0)))
    drawn = jax.random.truncated_normal(key_start, -6.0, 6.0, (RESPONSE_COUNT, RESPONSE_LENGTH, D), jnp.float32) * row_scale * column_scale
    return drawn.astype(jnp.bfloat16)


def block_levels(stream_key, dims, pieces, low, high):
    factor_of = 1.0
    for axis_at, parts in pieces:
        heights = jax.random.uniform(jax.random.fold_in(jax.random.fold_in(stream_key, 6), axis_at), (parts,), jnp.float32, low / len(pieces), high / len(pieces))
        factor_of = factor_of * jnp.repeat(jnp.exp(heights), dims[axis_at] // parts).reshape((-1,) + (1,) * (len(dims) - 1 - axis_at))
    return factor_of


def scatter_about(rng, shape, spread, bound, shards=(), held_as=jnp.bfloat16):
    gain = block_levels(rng, shape, shards, -0.22, 0.18) if shards else 1.0
    values = jax.random.normal(rng, shape, jnp.float32) * spread * gain
    return jnp.minimum(jnp.maximum(values, -bound), bound).astype(held_as)


def setup_inputs(seed: int = 0, part: int = 0) -> dict:
    splits = jax.random.split(jax.random.key(seed), 6)
    part_splits = jax.random.split(jax.random.fold_in(splits[5], part), 6)
    queries = draw_queries(jax.random.fold_in(jax.random.fold_in(splits[5], part), 71), part)
    keys = draw_keys(jax.random.fold_in(jax.random.fold_in(splits[5], part), 71), part)
    values = scatter_about(part_splits[2], (RESPONSE_COUNT, RESPONSE_LENGTH, KEY_VALUE_HEADS * HEAD_WIDTH), 4.0, 24.0, ((0, 2), (1, 8)))
    residual = draw_residual(jax.random.fold_in(jax.random.fold_in(splits[5], part), 71), part)
    norm_gain = jnp.clip(1.0 + 0.1 * jax.random.normal(splits[4], (D,), jnp.float32), 0.5, 1.5)
    return dict(queries=queries, keys=keys, values=values, residual=residual, norm_gain=norm_gain)


norm_eps = 1e-06

def reference(queries, keys, values, residual, norm_gain):
    queries_per_group = QUERY_HEADS // KEY_VALUE_HEADS
    position = jnp.arange(RESPONSE_LENGTH, dtype=jnp.int32)
    causal = position[None, :] <= position[:, None]

    def one_response(inputs):
        query_all, key_all, value_all = inputs

        def one_head(head_index):
            group_index = head_index // queries_per_group
            query_head = lax.dynamic_slice_in_dim(query_all, (head_index * HEAD_WIDTH).astype(jnp.int32), HEAD_WIDTH, 1)
            key_head = lax.dynamic_slice_in_dim(key_all, (group_index * HEAD_WIDTH).astype(jnp.int32), HEAD_WIDTH, 1)
            value_head = lax.dynamic_slice_in_dim(value_all, (group_index * HEAD_WIDTH).astype(jnp.int32), HEAD_WIDTH, 1)
            scores = jnp.dot(query_head, key_head.T, preferred_element_type=jnp.float32) * (1.0 / math.sqrt(HEAD_WIDTH))
            scores = jnp.where(causal, scores, -jnp.inf)
            row_max = lax.optimization_barrier(jnp.max(scores, axis=1, keepdims=True))
            weights = jnp.exp(scores - row_max)
            soft_probs = (weights / lax.optimization_barrier(jnp.sum(weights, axis=1, keepdims=True))).astype(jnp.bfloat16)
            return jnp.dot(soft_probs, value_head, preferred_element_type=jnp.float32).astype(jnp.bfloat16)
        heads_out = lax.map(one_head, jnp.arange(QUERY_HEADS, dtype=jnp.int32))
        return jnp.transpose(heads_out, (1, 0, 2)).reshape(RESPONSE_LENGTH, QUERY_HEADS * HEAD_WIDTH)
    attended = lax.map(one_response, (queries, keys, values))

    def one_norm(inputs):
        attended_rows, residual_rows = inputs
        hidden = residual_rows.astype(jnp.float32) + attended_rows.astype(jnp.float32)
        inv_rms = lax.rsqrt(lax.optimization_barrier(jnp.mean(hidden * hidden, axis=1, keepdims=True)) + norm_eps)
        return (hidden * inv_rms * norm_gain).astype(jnp.bfloat16)
    return lax.map(one_norm, (attended, residual))
```

```python
import functools
import math

import jax
import jax.numpy as jnp
from jax import lax
from jax.experimental import pallas as pl
from jax.experimental.pallas import tpu as pltpu
from jax.sharding import PartitionSpec as P

HEAD_WIDTH = 128
norm_eps = 1e-06
MESH = pl.DeviceIdType.MESH


def kernel(
    planes,
    rows,
    kv_heads,
    per_group,
    q_hbm,
    k_hbm,
    v_hbm,
    r_hbm,
    gain_hbm,
    out_ref,
    gain_ref,
    qbuf,
    rbuf,
    kvbuf,
    top,
    acc,
    squares,
    local_sem,
    own_sem,
    up_send,
    up_recv,
    side_send,
    side_recv,
    extra_send,
    extra_recv,
):
    W = HEAD_WIDTH
    heads = kv_heads * per_group
    width = heads * W
    me = lax.axis_index("seq")
    plane = me // 2
    col = lax.rem(me, 2)
    above = me + 2
    below = me - 2
    side = me + 1 - 2 * col
    has_up = plane + 1 < planes
    has_down = plane > 0
    factor = math.log2(math.e) / math.sqrt(W)

    barrier = pltpu.get_barrier_semaphore()

    @pl.when(has_down)
    def _():
        pl.semaphore_signal(barrier, inc=1, device_id={"seq": below}, device_id_type=MESH)

    pl.semaphore_signal(barrier, inc=1, device_id={"seq": side}, device_id_type=MESH)

    @pl.when(has_up)
    def _():
        pl.semaphore_signal(barrier, inc=1, device_id={"seq": above}, device_id_type=MESH)

    own = []
    for g in range(kv_heads):
        lanes = slice(g * W, (g + 1) * W)
        pair = (
            pltpu.make_async_copy(k_hbm.at[0, :, lanes], kvbuf.at[g, me, :, :W], own_sem.at[g, 0]),
            pltpu.make_async_copy(v_hbm.at[0, :, lanes], kvbuf.at[g, me, :, W:], own_sem.at[g, 1]),
        )
        for copy in pair:
            copy.start()
        own.append(pair)

    def query_copy(head):
        lanes = pl.ds(pl.multiple_of(head * W, W), W)
        return pltpu.make_async_copy(
            q_hbm.at[0, :, lanes], qbuf.at[head], local_sem.at[head]
        )

    r_in = pltpu.make_async_copy(r_hbm.at[0], rbuf, local_sem.at[heads])
    lax.fori_loop(0, heads, lambda head, carry: query_copy(head).start(), None)
    g_in = pltpu.make_async_copy(gain_hbm, gain_ref, local_sem.at[heads + 1])
    r_in.start()
    g_in.start()

    pl.semaphore_wait(barrier, 1 + has_up.astype(jnp.int32) + has_down.astype(jnp.int32))

    def remote(slot, send_sem, recv_sem, target):
        return pltpu.make_async_remote_copy(
            src_ref=slot,
            dst_ref=slot,
            send_sem=send_sem,
            recv_sem=recv_sem,
            device_id={"seq": target},
            device_id_type=MESH,
        )

    def up_copy(g, q):
        return remote(kvbuf.at[g, 2 * q + col], up_send.at[g, q], up_recv.at[g, q], above)

    def side_copy(g, q, column):
        return remote(kvbuf.at[g, 2 * q + column], side_send.at[g, q], side_recv.at[g, q], side)

    def extra_copy(g):
        return remote(kvbuf.at[g, 0], extra_send.at[g], extra_recv.at[g], above)

    def by_extra(g, q, column):
        return (column == 1) & (q == 0) & has_down & (lax.rem(g, 2) == 1)

    for g in range(kv_heads):
        for copy in own[g]:
            copy.wait()

        @pl.when(has_up)
        def _(g=g):
            up_copy(g, plane).start()

        @pl.when(col == 0)
        def _(g=g):
            side_copy(g, plane, col).start()

    squares[...] = jnp.zeros_like(squares)

    def relay(g, q):
        up_copy(g, q).wait_recv()

        @pl.when(has_up)
        def _():
            up_copy(g, q).start()

        @pl.when(jnp.logical_not(by_extra(g, q, 1 - col)))
        def _():
            side_copy(g, q, col).start()

    def attend(g, blocks, first):
        keys = jnp.concatenate([kvbuf[g, b, :, :W] for b in blocks], axis=0)
        vals = jnp.concatenate([kvbuf[g, b, :, W:] for b in blocks], axis=0)
        vals = jnp.concatenate([vals, jnp.ones_like(vals)], axis=1)
        size = len(blocks) * rows

        def scores(j):
            return lax.dot_general(
                qbuf[g * per_group + j],
                keys,
                (((1,), (1,)), ((), ())),
                preferred_element_type=jnp.float32,
            )

        def spread(x):
            tail = [x[:, : size % W]] if size % W else []
            return jnp.concatenate([x] * (size // W) + tail, axis=1)

        s_next = scores(0)
        for j in range(per_group):
            head = g * per_group + j
            s = s_next
            if j + 1 < per_group:
                s_next = scores(j + 1)
            if first:
                at_row = lax.broadcasted_iota(jnp.int32, s.shape, 0)
                at_key = lax.broadcasted_iota(jnp.int32, s.shape, 1)
                s = jnp.where(at_key <= at_row, s, -jnp.inf)
            wide = jnp.broadcast_to(jnp.max(s, axis=1, keepdims=True), (rows, W))
            if not first:
                old = top[head]
                wide = jnp.maximum(old, wide)
            s = (s - spread(wide)) * factor
            w = jnp.exp2(s).astype(jnp.bfloat16)
            o = jnp.dot(w, vals, preferred_element_type=jnp.float32)
            if not first:
                fade = jnp.exp2((old - wide) * factor)
                o = o + acc[head] * jnp.concatenate([fade, fade], axis=1)
            top[head] = wide
            acc[head] = o

    def finish(g):
        total = squares[...]
        for j in range(per_group):
            head = g * per_group + j
            lanes = pl.ds(pl.multiple_of(head * W, W), W)
            both = acc[head]
            attended = (both[:, :W] / both[:, W:]).astype(jnp.bfloat16).astype(jnp.float32)
            hidden = rbuf[:, lanes].astype(jnp.float32) + attended
            total = total + hidden * hidden
            top[head] = hidden
        squares[...] = total

    def diagonal(g, carry):
        lax.fori_loop(0, per_group, lambda j, inner: query_copy(g * per_group + j).wait(), None)
        attend(g, [me], True)
        return carry

    ahead = 2 * (1 - col)
    pieces = plane * kv_heads

    def relay_piece(i):
        relay(lax.rem(i, kv_heads), plane - 1 - i // kv_heads)

    lax.fori_loop(0, kv_heads, diagonal, 0)
    r_in.wait()
    g_in.wait()
    lax.fori_loop(0, jnp.minimum(ahead, pieces), lambda i, carry: relay_piece(i), None)

    @pl.when((col == 0) & (plane == 0))
    def _():
        lax.fori_loop(0, kv_heads, lambda g, carry: finish(g), None)

    @pl.when((col == 1) & has_up & (plane == 0))
    def _():
        for g in range(1, kv_heads, 2):
            side_copy(g, plane, 1 - col).wait_recv()
            extra_copy(g).start()

    def step(i, carry):
        g = lax.rem(i, kv_heads)
        q = plane - 1 - i // kv_heads

        @pl.when(i + ahead < pieces)
        def _():
            relay_piece(i + ahead)

        side_copy(g, q + col, 1 - col).wait_recv()
        attend(g, [2 * q + col, 2 * q + 1 + col], False)

        @pl.when((col == 0) & (q == 0))
        def _():
            finish(g)

        return carry

    lax.fori_loop(0, pieces, step, 0)

    def last(g, carry):
        @pl.when(by_extra(g, 0, col))
        def _():
            extra_copy(g).wait_recv()

        @pl.when(by_extra(g, 0, col) & has_up)
        def _():
            extra_copy(g).start()

        @pl.when(jnp.logical_not(by_extra(g, 0, col)) & (has_down | (lax.rem(g, 2) == 0) | jnp.logical_not(has_up)))
        def _():
            side_copy(g, 0, 0).wait_recv()

        attend(g, [0], False)
        finish(g)
        return carry

    @pl.when(col == 1)
    def _():
        lax.fori_loop(0, kv_heads, last, 0)

    mean = jnp.sum(squares[...], axis=1, keepdims=True) / width
    scale = jnp.broadcast_to(lax.rsqrt(mean + norm_eps), (rows, W))
    for head in range(kv_heads * per_group):
        lanes = slice(head * W, (head + 1) * W)
        gain = gain_ref[lanes].reshape(1, W)
        out_ref[0, :, lanes] = (top[head] * scale * gain).astype(jnp.bfloat16)

    def drain_own(g, carry):
        @pl.when(has_up)
        def _():
            up_copy(g, plane).wait_send()

        @pl.when(col == 0)
        def _():
            side_copy(g, plane, col).wait_send()

        @pl.when((col == 1) & has_up & (lax.rem(g, 2) == 1))
        def _():
            extra_copy(g).wait_send()

        return carry

    lax.fori_loop(0, kv_heads, drain_own, 0)

    def drain(q, carry):
        def one(g, inner):
            @pl.when(has_up)
            def _():
                up_copy(g, q).wait_send()

            @pl.when(jnp.logical_not(by_extra(g, q, 1 - col)))
            def _():
                side_copy(g, q, col).wait_send()

            return inner

        return lax.fori_loop(0, kv_heads, one, carry)

    lax.fori_loop(0, plane, drain, 0)


def body(queries, keys, values, residual, norm_gain):
    count = lax.axis_size("seq")
    rows = queries.shape[1]
    width = queries.shape[2]
    kv_heads = keys.shape[2] // HEAD_WIDTH
    heads = width // HEAD_WIDTH
    planes = count // 2
    queries, keys, values, residual, norm_gain = (
        pltpu.with_memory_space_constraint(x, pltpu.HBM)
        for x in (queries, keys, values, residual, norm_gain)
    )
    hbm = pl.BlockSpec(memory_space=pltpu.HBM)
    vmem = pl.BlockSpec(memory_space=pltpu.VMEM)
    return pl.pallas_call(
        functools.partial(kernel, planes, rows, kv_heads, heads // kv_heads),
        out_shape=pltpu.VMEM(queries.shape, jnp.bfloat16),
        in_specs=[hbm] * 5,
        out_specs=vmem,
        scratch_shapes=[
            pltpu.VMEM((width,), jnp.float32),
            pltpu.VMEM((heads, rows, HEAD_WIDTH), jnp.bfloat16),
            pltpu.VMEM((rows, width), jnp.bfloat16),
            pltpu.VMEM((kv_heads, count, rows, 2 * HEAD_WIDTH), jnp.bfloat16),
            pltpu.VMEM((heads, rows, HEAD_WIDTH), jnp.float32),
            pltpu.VMEM((heads, rows, 2 * HEAD_WIDTH), jnp.float32),
            pltpu.VMEM((rows, HEAD_WIDTH), jnp.float32),
            pltpu.SemaphoreType.DMA((heads + 2,)),
            pltpu.SemaphoreType.DMA((kv_heads, 2)),
            pltpu.SemaphoreType.DMA((kv_heads, planes)),
            pltpu.SemaphoreType.DMA((kv_heads, planes)),
            pltpu.SemaphoreType.DMA((kv_heads, planes)),
            pltpu.SemaphoreType.DMA((kv_heads, planes)),
            pltpu.SemaphoreType.DMA((kv_heads,)),
            pltpu.SemaphoreType.DMA((kv_heads,)),
        ],
        compiler_params=pltpu.CompilerParams(
            collective_id=0, has_side_effects=True, vmem_limit_bytes=54500000
        ),
    )(queries, keys, values, residual, norm_gain)


def solution(mesh):
    rows = P(("groups", "vocab", "batch"), "seq", None)
    return jax.shard_map(
        body,
        mesh=mesh,
        in_specs=(rows, rows, rows, rows, P()),
        out_specs=rows,
        check_vma=False,
    )
```

```python
import functools
import math

import jax
import jax.numpy as jnp
from jax import lax
from jax.experimental import pallas as pl
from jax.experimental.pallas import tpu as pltpu
from jax.sharding import PartitionSpec as P

HEAD_WIDTH = 128
norm_eps = 1e-06
MESH = pl.DeviceIdType.MESH


def kernel(
    planes,
    rows,
    kv_heads,
    per_group,
    q_hbm,
    k_hbm,
    v_hbm,
    r_hbm,
    gain_hbm,
    out_ref,
    gain_ref,
    qbuf,
    rbuf,
    kvbuf,
    top,
    acc,
    obuf,
    stat,
    squares,
    local_sem,
    own_sem,
    up_send,
    up_recv,
    side_send,
    side_recv,
    q3_send,
    q3_recv,
    o_send,
    o_recv,
):
    W = HEAD_WIDTH
    heads = kv_heads * per_group
    width = heads * W
    me = lax.axis_index("seq")
    plane = me // 2
    col = lax.rem(me, 2)
    above = me + 2
    below = me - 2
    side = me + 1 - 2 * col
    has_up = plane + 1 < planes
    has_down = plane > 0
    is_top = (plane == planes - 1) & (planes > 1)
    is_help = plane == planes - 2
    skip = is_top.astype(jnp.int32)
    factor = math.log2(math.e) / math.sqrt(W)

    barrier = pltpu.get_barrier_semaphore()

    @pl.when(has_down)
    def _():
        pl.semaphore_signal(barrier, inc=1, device_id={"seq": below}, device_id_type=MESH)

    pl.semaphore_signal(barrier, inc=1, device_id={"seq": side}, device_id_type=MESH)

    @pl.when(has_up)
    def _():
        pl.semaphore_signal(barrier, inc=1, device_id={"seq": above}, device_id_type=MESH)

    own = []
    for g in range(kv_heads):
        lanes = slice(g * W, (g + 1) * W)
        pair = (
            pltpu.make_async_copy(k_hbm.at[0, :, lanes], kvbuf.at[g, me, :, :W], own_sem.at[g, 0]),
            pltpu.make_async_copy(v_hbm.at[0, :, lanes], kvbuf.at[g, me, :, W:], own_sem.at[g, 1]),
        )
        for copy in pair:
            copy.start()
        own.append(pair)

    def query_copy(head):
        lanes = pl.ds(pl.multiple_of(head * W, W), W)
        return pltpu.make_async_copy(
            q_hbm.at[0, :, lanes], qbuf.at[head], local_sem.at[head]
        )

    r_in = pltpu.make_async_copy(r_hbm.at[0], rbuf, local_sem.at[heads])
    lax.fori_loop(0, heads, lambda head, carry: query_copy(head).start(), None)
    g_in = pltpu.make_async_copy(gain_hbm, gain_ref, local_sem.at[heads + 1])
    r_in.start()
    g_in.start()

    pl.semaphore_wait(barrier, 1 + has_up.astype(jnp.int32) + has_down.astype(jnp.int32))

    def remote(slot, send_sem, recv_sem, target):
        return pltpu.make_async_remote_copy(
            src_ref=slot,
            dst_ref=slot,
            send_sem=send_sem,
            recv_sem=recv_sem,
            device_id={"seq": target},
            device_id_type=MESH,
        )

    def up_copy(g, q):
        return remote(kvbuf.at[g, 2 * q + col], up_send.at[g, q], up_recv.at[g, q], above)

    def side_copy(g, q, column):
        return remote(kvbuf.at[g, 2 * q + column], side_send.at[g, q], side_recv.at[g, q], side)

    q3_copy = pltpu.make_async_remote_copy(
        src_ref=qbuf.at[pl.ds(0, per_group)],
        dst_ref=qbuf.at[pl.ds(heads, per_group)],
        send_sem=q3_send,
        recv_sem=q3_recv,
        device_id={"seq": below},
        device_id_type=MESH,
    )

    def o_copy(j):
        return remote(obuf.at[j], o_send.at[j], o_recv.at[j], above)

    stat_copy = remote(stat, o_send.at[per_group], o_recv.at[per_group], above)

    def goes_up(g):
        return has_up & jnp.logical_not(is_help & (g == 0))

    for g in range(kv_heads):
        for copy in own[g]:
            copy.wait()

        @pl.when(goes_up(g))
        def _(g=g):
            up_copy(g, plane).start()

        late = is_help & has_down if g >= 2 else False

        @pl.when((col == 0) & jnp.logical_not(late))
        def _(g=g):
            side_copy(g, plane, col).start()

        if g == 0:

            @pl.when((col == 1) & is_help)
            def _():
                side_copy(0, plane, col).start()

    squares[...] = jnp.zeros_like(squares)

    def relay(g, q):
        up_copy(g, q).wait_recv()

        @pl.when(goes_up(g))
        def _():
            up_copy(g, q).start()

        paced = is_help & (col == 0)

        @pl.when(jnp.logical_not(paced & (g >= 2) & (q >= 1)))
        def _():
            side_copy(g, q, col).start()

        @pl.when(paced & (g < 2) & (q == plane - 1))
        def _():
            side_copy(g + 2, plane, col).start()

        @pl.when(paced & (g == 0) & (q < plane - 1))
        def _():
            for h in range(2, kv_heads):
                side_copy(h, q + 1, col).start()

    def attend(base, g, blocks, first):
        keys = jnp.concatenate([kvbuf[g, b, :, :W] for b in blocks], axis=0)
        vals = jnp.concatenate([kvbuf[g, b, :, W:] for b in blocks], axis=0)
        vals = jnp.concatenate([vals, jnp.ones_like(vals)], axis=1)
        size = len(blocks) * rows

        def scores(j):
            return lax.dot_general(
                qbuf[base + j],
                keys,
                (((1,), (1,)), ((), ())),
                preferred_element_type=jnp.float32,
            )

        def spread(x):
            tail = [x[:, : size % W]] if size % W else []
            return jnp.concatenate([x] * (size // W) + tail, axis=1)

        s_next = scores(0)
        for j in range(per_group):
            head = base + j
            s = s_next
            if j + 1 < per_group:
                s_next = scores(j + 1)
            if first:
                at_row = lax.broadcasted_iota(jnp.int32, s.shape, 0)
                at_key = lax.broadcasted_iota(jnp.int32, s.shape, 1)
                s = jnp.where(at_key <= at_row, s, -jnp.inf)
            wide = jnp.broadcast_to(jnp.max(s, axis=1, keepdims=True), (rows, W))
            if not first:
                old = top[head]
                wide = jnp.maximum(old, wide)
            s = (s - spread(wide)) * factor
            w = jnp.exp2(s).astype(jnp.bfloat16)
            o = jnp.dot(w, vals, preferred_element_type=jnp.float32)
            if not first:
                fade = jnp.exp2((old - wide) * factor)
                o = o + acc[head] * jnp.concatenate([fade, fade], axis=1)
            top[head] = wide
            acc[head] = o

    def finish(g):
        total = squares[...]
        for j in range(per_group):
            head = g * per_group + j
            lanes = pl.ds(pl.multiple_of(head * W, W), W)
            both = acc[head]
            attended = (both[:, :W] / both[:, W:]).astype(jnp.bfloat16).astype(jnp.float32)
            hidden = rbuf[:, lanes].astype(jnp.float32) + attended
            total = total + hidden * hidden
            top[head] = hidden
        squares[...] = total

    def merge():
        total = squares[...]
        stat_copy.wait_recv()
        pad = jnp.zeros((W - stat.shape[0], stat.shape[1]), jnp.float32)
        far = jnp.transpose(jnp.concatenate([stat[...], pad], axis=0))[:rows]
        for j in range(per_group):
            lanes = slice(j * W, (j + 1) * W)
            o_copy(j).wait_recv()
            both = acc[j]
            near = top[j] * factor + jnp.log(both[:, W:]) * math.log2(math.e)
            share = 1.0 / (1.0 + jnp.exp2(near - jnp.broadcast_to(far[:, j : j + 1], (rows, W))))
            mine = both[:, :W] / both[:, W:]
            attended = mine + (obuf[j].astype(jnp.float32) - mine) * share
            attended = attended.astype(jnp.bfloat16).astype(jnp.float32)
            hidden = rbuf[:, lanes].astype(jnp.float32) + attended
            total = total + hidden * hidden
            top[j] = hidden
        squares[...] = total

    def emit():
        lane = lax.broadcasted_iota(jnp.int32, (rows, W), 1)
        far = jnp.zeros((rows, W), jnp.float32)
        for j in range(per_group):
            both = acc[heads + j]
            total = top[heads + j] * factor + jnp.log(both[:, W:]) * math.log2(math.e)
            far = jnp.where(lane == j, total, far)
            obuf[j] = (both[:, :W] / both[:, W:]).astype(jnp.bfloat16)
        pad = jnp.zeros((stat.shape[1] - rows, W), jnp.float32)
        stat[...] = jnp.transpose(jnp.concatenate([far, pad], axis=0))[: stat.shape[0]]

    def send_o():
        stat_copy.start()
        for j in range(per_group):
            o_copy(j).start()

    def helped(b, carry):
        @pl.when(b == plane)
        def _():
            q3_copy.wait_recv()

        @pl.when((b == plane) & ((col == 0) | (b == 0)))
        def _():
            side_copy(0, plane, 1 - col).wait_recv()

        @pl.when((col == 1) & (b < plane) & ((b == 0) | (b == 1)))
        def _():
            side_copy(0, b, 0).wait_recv()

        attend(heads, 0, [2 * b, 2 * b + 1], False)
        return carry

    def diagonal(g, carry):
        lax.fori_loop(0, per_group, lambda j, inner: query_copy(g * per_group + j).wait(), None)

        @pl.when(is_top & (g == 0))
        def _():
            q3_copy.start()

        attend(g * per_group, g, [me], True)
        return carry

    ahead = jnp.where((col == 0) | is_help, 2, 0)
    groups = kv_heads - skip
    pieces = plane * groups

    def relay_piece(i):
        relay(lax.rem(i, groups) + skip, plane - 1 - i // groups)

    lax.fori_loop(0, kv_heads, diagonal, 0)
    r_in.wait()
    g_in.wait()
    lax.fori_loop(0, jnp.minimum(ahead, pieces), lambda i, carry: relay_piece(i), None)

    @pl.when(is_help)
    def _():
        top[pl.ds(heads, per_group)] = jnp.full((per_group, rows, W), -1e30, jnp.float32)
        acc[pl.ds(heads, per_group)] = jnp.zeros((per_group, rows, 2 * W), jnp.float32)

    @pl.when(is_help & (plane == 0))
    def _():
        lax.fori_loop(0, 1, helped, 0)
        emit()
        send_o()

    @pl.when((col == 0) & (plane == 0))
    def _():
        lax.fori_loop(0, kv_heads, lambda g, carry: finish(g), None)

    def step(i, carry):
        g = lax.rem(i, groups) + skip
        q = plane - 1 - i // groups

        @pl.when((i + ahead < pieces) & jnp.logical_not(is_help & (i + ahead == pieces - 1)))
        def _():
            relay_piece(i + ahead)

        @pl.when(jnp.logical_not(is_help & (col == 1) & (q == 0) & (g == 0) & (plane > 1)))
        def _():
            side_copy(g, q + col, 1 - col).wait_recv()

        final = is_help & (q == 0) & (g == 0)
        whole = is_help & (g == kv_heads - 2) & (q >= 1)
        second = is_help & (g == kv_heads - 1) & (q == 1)
        low = jnp.where(whole, q + 1, jnp.where(second, 1, 0))
        many = jnp.where(final, jnp.where(plane == 1, 2, 1), (whole | second).astype(jnp.int32))
        lax.fori_loop(low, low + many, helped, 0)

        @pl.when(final)
        def _():
            emit()
            relay_piece(pieces - 1)
            send_o()

        attend(g * per_group, g, [2 * q + col, 2 * q + 1 + col], False)

        @pl.when((col == 0) & (q == 0))
        def _():
            finish(g)

        return carry

    lax.fori_loop(0, pieces, step, 0)

    def last(g, carry):
        q = jnp.where(is_top & (g == 0), plane, 0)

        @pl.when(jnp.logical_not(is_help & (g == 0)))
        def _():
            side_copy(g, q, 0).wait_recv()

        attend(g * per_group, g, [2 * q], False)

        @pl.when(jnp.logical_not(is_top & (g == 0)))
        def _():
            finish(g)

        return carry

    @pl.when(col == 1)
    def _():
        lax.fori_loop(0, kv_heads, last, 0)

    @pl.when(is_top)
    def _():
        merge()

    mean = jnp.sum(squares[...], axis=1, keepdims=True) / width
    scale = jnp.broadcast_to(lax.rsqrt(mean + norm_eps), (rows, W))
    for head in range(kv_heads * per_group):
        lanes = slice(head * W, (head + 1) * W)
        gain = gain_ref[lanes].reshape(1, W)
        out_ref[0, :, lanes] = (top[head] * scale * gain).astype(jnp.bfloat16)

    def drain_own(g, carry):
        @pl.when(goes_up(g))
        def _():
            up_copy(g, plane).wait_send()

        @pl.when((col == 0) | (is_help & (g == 0)))
        def _():
            side_copy(g, plane, col).wait_send()

        return carry

    lax.fori_loop(0, kv_heads, drain_own, 0)

    def drain(q, carry):
        def one(g, inner):
            @pl.when(goes_up(g))
            def _():
                up_copy(g, q).wait_send()

            side_copy(g, q, col).wait_send()
            return inner

        return lax.fori_loop(skip, kv_heads, one, carry)

    lax.fori_loop(0, plane, drain, 0)

    @pl.when(is_top)
    def _():
        q3_copy.wait_send()

    @pl.when(is_help)
    def _():
        stat_copy.wait_send()
        for j in range(per_group):
            o_copy(j).wait_send()


def body(queries, keys, values, residual, norm_gain):
    count = lax.axis_size("seq")
    rows = queries.shape[1]
    width = queries.shape[2]
    kv_heads = keys.shape[2] // HEAD_WIDTH
    heads = width // HEAD_WIDTH
    planes = count // 2
    per_group = heads // kv_heads
    queries, keys, values, residual, norm_gain = (
        pltpu.with_memory_space_constraint(x, pltpu.HBM)
        for x in (queries, keys, values, residual, norm_gain)
    )
    hbm = pl.BlockSpec(memory_space=pltpu.HBM)
    vmem = pl.BlockSpec(memory_space=pltpu.VMEM)
    return pl.pallas_call(
        functools.partial(kernel, planes, rows, kv_heads, per_group),
        out_shape=pltpu.VMEM(queries.shape, jnp.bfloat16),
        in_specs=[hbm] * 5,
        out_specs=vmem,
        scratch_shapes=[
            pltpu.VMEM((width,), jnp.float32),
            pltpu.VMEM((heads + per_group, rows, HEAD_WIDTH), jnp.bfloat16),
            pltpu.VMEM((rows, width), jnp.bfloat16),
            pltpu.VMEM((kv_heads, count, rows, 2 * HEAD_WIDTH), jnp.bfloat16),
            pltpu.VMEM((heads + per_group, rows, HEAD_WIDTH), jnp.float32),
            pltpu.VMEM((heads + per_group, rows, 2 * HEAD_WIDTH), jnp.float32),
            pltpu.VMEM((per_group, rows, HEAD_WIDTH), jnp.bfloat16),
            pltpu.VMEM((-(-per_group // 8) * 8, -(-rows // HEAD_WIDTH) * HEAD_WIDTH), jnp.float32),
            pltpu.VMEM((rows, HEAD_WIDTH), jnp.float32),
            pltpu.SemaphoreType.DMA((heads + 2,)),
            pltpu.SemaphoreType.DMA((kv_heads, 2)),
            pltpu.SemaphoreType.DMA((kv_heads, planes)),
            pltpu.SemaphoreType.DMA((kv_heads, planes)),
            pltpu.SemaphoreType.DMA((kv_heads, planes)),
            pltpu.SemaphoreType.DMA((kv_heads, planes)),
            pltpu.SemaphoreType.DMA,
            pltpu.SemaphoreType.DMA,
            pltpu.SemaphoreType.DMA((per_group + 1,)),
            pltpu.SemaphoreType.DMA((per_group + 1,)),
        ],
        compiler_params=pltpu.CompilerParams(
            collective_id=0, has_side_effects=True, vmem_limit_bytes=54500000
        ),
    )(queries, keys, values, residual, norm_gain)


def solution(mesh):
    rows = P(("groups", "vocab", "batch"), "seq", None)
    return jax.shard_map(
        body,
        mesh=mesh,
        in_specs=(rows, rows, rows, rows, P()),
        out_specs=rows,
        check_vma=False,
    )
```

```python
import functools
import math

import jax
import jax.numpy as jnp
from jax import lax
from jax.experimental import pallas as pl
from jax.experimental.pallas import tpu as pltpu
from jax.sharding import PartitionSpec as P

HEAD_WIDTH = 128
norm_eps = 1e-06
MESH = pl.DeviceIdType.MESH


def kernel(
    planes,
    rows,
    kv_heads,
    per_group,
    q_hbm,
    k_hbm,
    v_hbm,
    r_hbm,
    gain_hbm,
    out_ref,
    gain_ref,
    qbuf,
    rbuf,
    kvbuf,
    top,
    acc,
    obuf,
    stat,
    squares,
    local_sem,
    own_sem,
    up_send,
    up_recv,
    side_send,
    side_recv,
    q3_send,
    q3_recv,
    o_send,
    o_recv,
    x_send,
    x_recv,
):
    W = HEAD_WIDTH
    heads = kv_heads * per_group
    width = heads * W
    me = lax.axis_index("seq")
    plane = me // 2
    col = lax.rem(me, 2)
    above = me + 2
    below = me - 2
    side = me + 1 - 2 * col
    has_up = plane + 1 < planes
    has_down = plane > 0
    is_top = (plane == planes - 1) & (planes > 1)
    is_help = plane == planes - 2
    skip = is_top.astype(jnp.int32)
    factor = math.log2(math.e) / math.sqrt(W)

    barrier = pltpu.get_barrier_semaphore()

    @pl.when(has_down)
    def _():
        pl.semaphore_signal(barrier, inc=1, device_id={"seq": below}, device_id_type=MESH)

    pl.semaphore_signal(barrier, inc=1, device_id={"seq": side}, device_id_type=MESH)

    @pl.when(has_up)
    def _():
        pl.semaphore_signal(barrier, inc=1, device_id={"seq": above}, device_id_type=MESH)

    own = []
    for g in range(kv_heads):
        lanes = slice(g * W, (g + 1) * W)
        pair = (
            pltpu.make_async_copy(k_hbm.at[0, :, lanes], kvbuf.at[g, me, :, :W], own_sem.at[g, 0]),
            pltpu.make_async_copy(v_hbm.at[0, :, lanes], kvbuf.at[g, me, :, W:], own_sem.at[g, 1]),
        )
        for copy in pair:
            copy.start()
        own.append(pair)

    def query_copy(head):
        lanes = pl.ds(pl.multiple_of(head * W, W), W)
        return pltpu.make_async_copy(
            q_hbm.at[0, :, lanes], qbuf.at[head], local_sem.at[head]
        )

    r_in = pltpu.make_async_copy(r_hbm.at[0], rbuf, local_sem.at[heads])
    lax.fori_loop(0, heads, lambda head, carry: query_copy(head).start(), None)
    g_in = pltpu.make_async_copy(gain_hbm, gain_ref, local_sem.at[heads + 1])
    r_in.start()
    g_in.start()

    pl.semaphore_wait(barrier, 1 + has_up.astype(jnp.int32) + has_down.astype(jnp.int32))

    def remote(slot, send_sem, recv_sem, target):
        return pltpu.make_async_remote_copy(
            src_ref=slot,
            dst_ref=slot,
            send_sem=send_sem,
            recv_sem=recv_sem,
            device_id={"seq": target},
            device_id_type=MESH,
        )

    def up_copy(g, q):
        return remote(kvbuf.at[g, 2 * q + col], up_send.at[g, q], up_recv.at[g, q], above)

    def side_copy(g, q, column):
        return remote(kvbuf.at[g, 2 * q + column], side_send.at[g, q], side_recv.at[g, q], side)

    half = rows // 2
    use_detour = planes > 3
    detour_g = 1

    def half_side(g, q):
        slot = kvbuf.at[g, 2 * q, pl.ds(0, half)]
        return remote(slot, side_send.at[g, q], side_recv.at[g, q], side)

    def detour(q):
        slot = kvbuf.at[detour_g, 2 * q, pl.ds(half, half)]
        return remote(slot, x_send, x_recv, above)

    def by_detour(g, q, column):
        return use_detour & is_top & (q == plane - 2) & (g == detour_g) & (column == 0)

    q3_copy = pltpu.make_async_remote_copy(
        src_ref=qbuf.at[pl.ds(0, per_group)],
        dst_ref=qbuf.at[pl.ds(heads, per_group)],
        send_sem=q3_send,
        recv_sem=q3_recv,
        device_id={"seq": below},
        device_id_type=MESH,
    )

    def o_copy(j):
        return remote(obuf.at[j], o_send.at[j], o_recv.at[j], above)

    stat_copy = remote(stat, o_send.at[per_group], o_recv.at[per_group], above)

    def goes_up(g):
        return has_up & jnp.logical_not(is_help & (g == 0))

    for g in range(kv_heads):
        for copy in own[g]:
            copy.wait()

        @pl.when(goes_up(g))
        def _(g=g):
            up_copy(g, plane).start()

        late = is_help & has_down if g >= 2 else False

        @pl.when((col == 0) & jnp.logical_not(late))
        def _(g=g):
            side_copy(g, plane, col).start()

        if g == 0:

            @pl.when((col == 1) & is_help)
            def _():
                side_copy(0, plane, col).start()

    @pl.when(is_top)
    def _():
        lax.fori_loop(0, per_group, lambda j, inner: query_copy(j).wait(), None)
        q3_copy.start()

    squares[...] = jnp.zeros_like(squares)

    def relay(g, q):
        up_copy(g, q).wait_recv()

        @pl.when(goes_up(g))
        def _():
            up_copy(g, q).start()

        paced = is_help & (col == 0)

        @pl.when(by_detour(g, q, col))
        def _():
            half_side(g, q).start()

        @pl.when(jnp.logical_not((paced & (g >= 2) & (q >= 1)) | by_detour(g, q, col)))
        def _():
            side_copy(g, q, col).start()

        @pl.when(paced & (g < 2) & (q == plane - 1))
        def _():
            side_copy(g + 2, plane, col).start()

        @pl.when(paced & (g == 0) & (q < plane - 1))
        def _():
            for h in range(2, kv_heads):
                side_copy(h, q + 1, col).start()

    def attend(base, g, blocks, first):
        keys = jnp.concatenate([kvbuf[g, b, :, :W] for b in blocks], axis=0)
        vals = jnp.concatenate([kvbuf[g, b, :, W:] for b in blocks], axis=0)
        vals = jnp.concatenate([vals, jnp.ones_like(vals)], axis=1)
        size = len(blocks) * rows

        def scores(j):
            return lax.dot_general(
                qbuf[base + j],
                keys,
                (((1,), (1,)), ((), ())),
                preferred_element_type=jnp.float32,
            )

        def spread(x):
            tail = [x[:, : size % W]] if size % W else []
            return jnp.concatenate([x] * (size // W) + tail, axis=1)

        s_next = scores(0)
        for j in range(per_group):
            head = base + j
            s = s_next
            if j + 1 < per_group:
                s_next = scores(j + 1)
            if first:
                at_row = lax.broadcasted_iota(jnp.int32, s.shape, 0)
                at_key = lax.broadcasted_iota(jnp.int32, s.shape, 1)
                s = jnp.where(at_key <= at_row, s, -jnp.inf)
            wide = jnp.broadcast_to(jnp.max(s, axis=1, keepdims=True), (rows, W))
            if not first:
                old = top[head]
                wide = jnp.maximum(old, wide)
            s = (s - spread(wide)) * factor
            w = jnp.exp2(s).astype(jnp.bfloat16)
            o = jnp.dot(w, vals, preferred_element_type=jnp.float32)
            if not first:
                fade = jnp.exp2((old - wide) * factor)
                o = o + acc[head] * jnp.concatenate([fade, fade], axis=1)
            top[head] = wide
            acc[head] = o

    def finish(g):
        total = squares[...]
        for j in range(per_group):
            head = g * per_group + j
            lanes = pl.ds(pl.multiple_of(head * W, W), W)
            both = acc[head]
            attended = (both[:, :W] / both[:, W:]).astype(jnp.bfloat16).astype(jnp.float32)
            hidden = rbuf[:, lanes].astype(jnp.float32) + attended
            total = total + hidden * hidden
            top[head] = hidden
        squares[...] = total

    def merge(first, end):
        total = squares[...]
        if first == 0:
            stat_copy.wait_recv()
        pad = jnp.zeros((W - stat.shape[0], stat.shape[1]), jnp.float32)
        far = jnp.transpose(jnp.concatenate([stat[...], pad], axis=0))[:rows]
        for j in range(first, end):
            lanes = slice(j * W, (j + 1) * W)
            o_copy(j).wait_recv()
            both = acc[j]
            near = top[j] * factor + jnp.log(both[:, W:]) * math.log2(math.e)
            share = 1.0 / (1.0 + jnp.exp2(near - jnp.broadcast_to(far[:, j : j + 1], (rows, W))))
            mine = both[:, :W] / both[:, W:]
            attended = mine + (obuf[j].astype(jnp.float32) - mine) * share
            attended = attended.astype(jnp.bfloat16).astype(jnp.float32)
            hidden = rbuf[:, lanes].astype(jnp.float32) + attended
            total = total + hidden * hidden
            top[j] = hidden
        squares[...] = total

    def emit():
        lane = lax.broadcasted_iota(jnp.int32, (rows, W), 1)
        far = jnp.zeros((rows, W), jnp.float32)
        for j in range(per_group):
            both = acc[heads + j]
            total = top[heads + j] * factor + jnp.log(both[:, W:]) * math.log2(math.e)
            far = jnp.where(lane == j, total, far)
            obuf[j] = (both[:, :W] / both[:, W:]).astype(jnp.bfloat16)
        pad = jnp.zeros((stat.shape[1] - rows, W), jnp.float32)
        stat[...] = jnp.transpose(jnp.concatenate([far, pad], axis=0))[: stat.shape[0]]

    def send_o():
        stat_copy.start()
        for j in range(per_group):
            o_copy(j).start()

    def helped(b, carry):
        @pl.when(b == plane)
        def _():
            q3_copy.wait_recv()

        @pl.when((b == plane) & ((col == 0) | (b == 0)))
        def _():
            side_copy(0, plane, 1 - col).wait_recv()

        @pl.when((col == 1) & (b < plane) & ((b == 0) | (b == 1)))
        def _():
            side_copy(0, b, 0).wait_recv()

        attend(heads, 0, [2 * b, 2 * b + 1], False)
        return carry

    def diagonal(g, carry):
        @pl.when(jnp.logical_not(is_top & (g == 0)))
        def _():
            lax.fori_loop(0, per_group, lambda j, inner: query_copy(g * per_group + j).wait(), None)

        attend(g * per_group, g, [me], True)
        return carry

    ahead = jnp.where((col == 0) | is_help, 2, 0)
    groups = kv_heads - skip
    pieces = plane * groups

    def relay_piece(i):
        relay(lax.rem(i, groups) + skip, plane - 1 - i // groups)

    lax.fori_loop(0, kv_heads, diagonal, 0)
    r_in.wait()
    g_in.wait()
    lax.fori_loop(0, jnp.minimum(ahead, pieces), lambda i, carry: relay_piece(i), None)

    @pl.when(is_help)
    def _():
        top[pl.ds(heads, per_group)] = jnp.full((per_group, rows, W), -1e30, jnp.float32)
        acc[pl.ds(heads, per_group)] = jnp.zeros((per_group, rows, 2 * W), jnp.float32)

    @pl.when(is_help & (plane == 0))
    def _():
        lax.fori_loop(0, 1, helped, 0)
        emit()
        send_o()

    @pl.when((col == 0) & (plane == 0))
    def _():
        lax.fori_loop(0, kv_heads, lambda g, carry: finish(g), None)

    def paired(i, carry):
        g = lax.rem(i, groups) + skip
        q = plane - 1 - i // groups
        attend(g * per_group, g, [2 * q + col, 2 * q + 1 + col], False)
        return carry

    def step(i, carry):
        g = lax.rem(i, groups) + skip
        q = plane - 1 - i // groups

        @pl.when((i + ahead < pieces) & jnp.logical_not(is_help & (i + ahead == pieces - 1)))
        def _():
            relay_piece(i + ahead)

        there = by_detour(g, q + col, 1 - col)

        @pl.when(there)
        def _():
            half_side(g, q + col).wait_recv()
            detour(q + col).wait_recv()

        had = ((g == 0) & (q == 0) & (plane > 1)) | (use_detour & (g == detour_g) & (q == plane - 2))

        @pl.when(jnp.logical_not((is_help & (col == 1) & had) | there))
        def _():
            side_copy(g, q + col, 1 - col).wait_recv()

        @pl.when(use_detour & is_help & (col == 1) & (q == plane - 1) & (g == detour_g + 1))
        def _():
            side_copy(detour_g, q, 0).wait_recv()
            detour(q).start()

        final = is_help & (q == 0) & (g == 0)
        whole = is_help & (g == kv_heads - 2) & (q >= 1)
        second = is_help & (g == kv_heads - 1) & (q == 1)
        low = jnp.where(whole, q + 1, jnp.where(second, 1, 0))
        many = jnp.where(final, jnp.where(plane == 1, 2, 1), (whole | second).astype(jnp.int32))
        lax.fori_loop(low, low + many, helped, 0)

        @pl.when(final)
        def _():
            emit()
            relay_piece(pieces - 1)
            send_o()

        later = is_help & (q == 1) & (g == kv_heads - 1)
        start = jnp.where(final & (plane > 1), i - 1, i)
        lax.fori_loop(start, jnp.where(later, start, i + 1), paired, 0)

        @pl.when((col == 0) & (q == 0))
        def _():
            finish(g)

        return carry

    lax.fori_loop(0, pieces, step, 0)

    early = per_group - 2

    def last(g, carry):
        q = jnp.where(is_top & (g == 0), plane, 0)

        @pl.when(is_top & (g == kv_heads - 1))
        def _():
            merge(0, early)

        @pl.when(jnp.logical_not(is_help & (g == 0)))
        def _():
            side_copy(g, q, 0).wait_recv()

        attend(g * per_group, g, [2 * q], False)

        @pl.when(jnp.logical_not(is_top & (g == 0)))
        def _():
            finish(g)

        return carry

    @pl.when(col == 1)
    def _():
        lax.fori_loop(0, kv_heads, last, 0)

    @pl.when(is_top & (col == 0))
    def _():
        merge(0, early)

    @pl.when(is_top)
    def _():
        merge(early, per_group)

    mean = jnp.sum(squares[...], axis=1, keepdims=True) / width
    scale = jnp.broadcast_to(lax.rsqrt(mean + norm_eps), (rows, W))
    for head in range(kv_heads * per_group):
        lanes = slice(head * W, (head + 1) * W)
        gain = gain_ref[lanes].reshape(1, W)
        out_ref[0, :, lanes] = (top[head] * scale * gain).astype(jnp.bfloat16)

    def drain_own(g, carry):
        @pl.when(goes_up(g))
        def _():
            up_copy(g, plane).wait_send()

        @pl.when((col == 0) | (is_help & (g == 0)))
        def _():
            side_copy(g, plane, col).wait_send()

        return carry

    lax.fori_loop(0, kv_heads, drain_own, 0)

    def drain(q, carry):
        def one(g, inner):
            @pl.when(goes_up(g))
            def _():
                up_copy(g, q).wait_send()

            @pl.when(by_detour(g, q, col))
            def _():
                half_side(g, q).wait_send()

            @pl.when(jnp.logical_not(by_detour(g, q, col)))
            def _():
                side_copy(g, q, col).wait_send()

            return inner

        return lax.fori_loop(skip, kv_heads, one, carry)

    lax.fori_loop(0, plane, drain, 0)

    @pl.when(is_top)
    def _():
        q3_copy.wait_send()

    @pl.when(is_help)
    def _():
        stat_copy.wait_send()

        @pl.when(use_detour & (col == 1))
        def _():
            detour(plane - 1).wait_send()

        for j in range(per_group):
            o_copy(j).wait_send()


def body(queries, keys, values, residual, norm_gain):
    count = lax.axis_size("seq")
    rows = queries.shape[1]
    width = queries.shape[2]
    kv_heads = keys.shape[2] // HEAD_WIDTH
    heads = width // HEAD_WIDTH
    planes = count // 2
    per_group = heads // kv_heads
    queries, keys, values, residual, norm_gain = (
        pltpu.with_memory_space_constraint(x, pltpu.HBM)
        for x in (queries, keys, values, residual, norm_gain)
    )
    hbm = pl.BlockSpec(memory_space=pltpu.HBM)
    vmem = pl.BlockSpec(memory_space=pltpu.VMEM)
    return pl.pallas_call(
        functools.partial(kernel, planes, rows, kv_heads, per_group),
        out_shape=pltpu.VMEM(queries.shape, jnp.bfloat16),
        in_specs=[hbm] * 5,
        out_specs=vmem,
        scratch_shapes=[
            pltpu.VMEM((width,), jnp.float32),
            pltpu.VMEM((heads + per_group, rows, HEAD_WIDTH), jnp.bfloat16),
            pltpu.VMEM((rows, width), jnp.bfloat16),
            pltpu.VMEM((kv_heads, count, rows, 2 * HEAD_WIDTH), jnp.bfloat16),
            pltpu.VMEM((heads + per_group, rows, HEAD_WIDTH), jnp.float32),
            pltpu.VMEM((heads + per_group, rows, 2 * HEAD_WIDTH), jnp.float32),
            pltpu.VMEM((per_group, rows, HEAD_WIDTH), jnp.bfloat16),
            pltpu.VMEM((-(-per_group // 8) * 8, -(-rows // HEAD_WIDTH) * HEAD_WIDTH), jnp.float32),
            pltpu.VMEM((rows, HEAD_WIDTH), jnp.float32),
            pltpu.SemaphoreType.DMA((heads + 2,)),
            pltpu.SemaphoreType.DMA((kv_heads, 2)),
            pltpu.SemaphoreType.DMA((kv_heads, planes)),
            pltpu.SemaphoreType.DMA((kv_heads, planes)),
            pltpu.SemaphoreType.DMA((kv_heads, planes)),
            pltpu.SemaphoreType.DMA((kv_heads, planes)),
            pltpu.SemaphoreType.DMA,
            pltpu.SemaphoreType.DMA,
            pltpu.SemaphoreType.DMA((per_group + 1,)),
            pltpu.SemaphoreType.DMA((per_group + 1,)),
            pltpu.SemaphoreType.DMA,
            pltpu.SemaphoreType.DMA,
        ],
        compiler_params=pltpu.CompilerParams(
            collective_id=0, has_side_effects=True, vmem_limit_bytes=54500000
        ),
    )(queries, keys, values, residual, norm_gain)


def solution(mesh):
    rows = P(("groups", "vocab", "batch"), "seq", None)
    return jax.shard_map(
        body,
        mesh=mesh,
        in_specs=(rows, rows, rows, rows, P()),
        out_specs=rows,
        check_vma=False,
    )
```

```python
import functools
import math

import jax
import jax.numpy as jnp
from jax import lax
from jax.experimental import pallas as pl
from jax.experimental.pallas import tpu as pltpu
from jax.sharding import PartitionSpec as P

HEAD_WIDTH = 128
norm_eps = 1e-06
MESH = pl.DeviceIdType.MESH


def kernel(
    planes,
    rows,
    kv_heads,
    per_group,
    q_hbm,
    k_hbm,
    v_hbm,
    r_hbm,
    gain_hbm,
    out_ref,
    gain_ref,
    qbuf,
    rbuf,
    kvbuf,
    top,
    acc,
    obuf,
    stat,
    squares,
    local_sem,
    own_sem,
    up_send,
    up_recv,
    side_send,
    side_recv,
    q3_send,
    q3_recv,
    o_send,
    o_recv,
    x_send,
    x_recv,
):
    W = HEAD_WIDTH
    heads = kv_heads * per_group
    width = heads * W
    me = lax.axis_index("seq")
    plane = me // 2
    col = lax.rem(me, 2)
    above = me + 2
    below = me - 2
    side = me + 1 - 2 * col
    has_up = plane + 1 < planes
    has_down = plane > 0
    is_top = (plane == planes - 1) & (planes > 1)
    is_help = plane == planes - 2
    skip = is_top.astype(jnp.int32)
    factor = math.log2(math.e) / math.sqrt(W)

    barrier = pltpu.get_barrier_semaphore()

    @pl.when(has_down)
    def _():
        pl.semaphore_signal(barrier, inc=1, device_id={"seq": below}, device_id_type=MESH)

    pl.semaphore_signal(barrier, inc=1, device_id={"seq": side}, device_id_type=MESH)

    @pl.when(has_up)
    def _():
        pl.semaphore_signal(barrier, inc=1, device_id={"seq": above}, device_id_type=MESH)

    own = []
    for g in range(kv_heads):
        lanes = slice(g * W, (g + 1) * W)
        pair = (
            pltpu.make_async_copy(k_hbm.at[0, :, lanes], kvbuf.at[g, me, :, :W], own_sem.at[g, 0]),
            pltpu.make_async_copy(v_hbm.at[0, :, lanes], kvbuf.at[g, me, :, W:], own_sem.at[g, 1]),
        )
        for copy in pair:
            copy.start()
        own.append(pair)

    def query_copy(head):
        lanes = pl.ds(pl.multiple_of(head * W, W), W)
        return pltpu.make_async_copy(
            q_hbm.at[0, :, lanes], qbuf.at[head], local_sem.at[head]
        )

    r_in = pltpu.make_async_copy(r_hbm.at[0], rbuf, local_sem.at[heads])
    lax.fori_loop(0, heads, lambda head, carry: query_copy(head).start(), None)
    g_in = pltpu.make_async_copy(gain_hbm, gain_ref, local_sem.at[heads + 1])
    r_in.start()
    g_in.start()

    pl.semaphore_wait(barrier, 1 + has_up.astype(jnp.int32) + has_down.astype(jnp.int32))

    def remote(slot, send_sem, recv_sem, target):
        return pltpu.make_async_remote_copy(
            src_ref=slot,
            dst_ref=slot,
            send_sem=send_sem,
            recv_sem=recv_sem,
            device_id={"seq": target},
            device_id_type=MESH,
        )

    def up_copy(g, q):
        return remote(kvbuf.at[g, 2 * q + col], up_send.at[g, q], up_recv.at[g, q], above)

    def side_copy(g, q, column):
        return remote(kvbuf.at[g, 2 * q + column], side_send.at[g, q], side_recv.at[g, q], side)

    half = rows // 2
    use_detour = planes > 3
    detour_g = 1

    def half_side(g, q):
        slot = kvbuf.at[g, 2 * q, pl.ds(0, half)]
        return remote(slot, side_send.at[g, q], side_recv.at[g, q], side)

    def detour(q):
        slot = kvbuf.at[detour_g, 2 * q, pl.ds(half, half)]
        return remote(slot, x_send, x_recv, above)

    def by_detour(g, q, column):
        return use_detour & is_top & (q == plane - 2) & (g == detour_g) & (column == 0)

    q3_copy = pltpu.make_async_remote_copy(
        src_ref=qbuf.at[pl.ds(0, per_group)],
        dst_ref=qbuf.at[pl.ds(heads, per_group)],
        send_sem=q3_send,
        recv_sem=q3_recv,
        device_id={"seq": below},
        device_id_type=MESH,
    )

    def o_copy(j):
        return remote(obuf.at[j], o_send.at[j], o_recv.at[j], above)

    stat_copy = remote(stat, o_send.at[per_group], o_recv.at[per_group], above)

    def goes_up(g):
        return has_up & jnp.logical_not(is_help & (g == 0))

    for g in range(kv_heads):
        for copy in own[g]:
            copy.wait()

        @pl.when(goes_up(g))
        def _(g=g):
            up_copy(g, plane).start()

        late = is_help & has_down if g >= 2 else False

        @pl.when((col == 0) & jnp.logical_not(late))
        def _(g=g):
            side_copy(g, plane, col).start()

        if g == 0:

            @pl.when((col == 1) & is_help)
            def _():
                side_copy(0, plane, col).start()

    @pl.when(is_top)
    def _():
        lax.fori_loop(0, per_group, lambda j, inner: query_copy(j).wait(), None)
        q3_copy.start()

    squares[...] = jnp.zeros_like(squares)

    def relay(g, q):
        up_copy(g, q).wait_recv()

        @pl.when(goes_up(g))
        def _():
            up_copy(g, q).start()

        paced = is_help & (col == 0)

        @pl.when(by_detour(g, q, col))
        def _():
            half_side(g, q).start()

        @pl.when(jnp.logical_not((paced & (g >= 2) & (q >= 1)) | by_detour(g, q, col)))
        def _():
            side_copy(g, q, col).start()

        @pl.when(paced & (g < 2) & (q == plane - 1))
        def _():
            side_copy(g + 2, plane, col).start()

        @pl.when(paced & (g == 0) & (q < plane - 1))
        def _():
            for h in range(2, kv_heads):
                side_copy(h, q + 1, col).start()

    def attend(base, g, blocks, first):
        keys = jnp.concatenate([kvbuf[g, b, :, :W] for b in blocks], axis=0)
        vals = jnp.concatenate([kvbuf[g, b, :, W:] for b in blocks], axis=0)
        vals = jnp.concatenate([vals, jnp.ones_like(vals)], axis=1)
        size = len(blocks) * rows

        packs = [(at, min(3, per_group - at)) for at in range(0, per_group, 3)]

        def scores(k):
            at, count = packs[k]
            return lax.dot_general(
                qbuf[pl.ds(base + at, count)].reshape(count * rows, W),
                keys,
                (((1,), (1,)), ((), ())),
                preferred_element_type=jnp.float32,
            )

        def spread(x):
            tail = [x[:, : size % W]] if size % W else []
            return jnp.concatenate([x] * (size // W) + tail, axis=1)

        s_next = scores(0)
        for k, (at, count) in enumerate(packs):
            head = pl.ds(base + at, count)
            tall = count * rows
            s = s_next
            if k + 1 < len(packs):
                s_next = scores(k + 1)
            if first:
                at_row = lax.broadcasted_iota(jnp.int32, (rows, size), 0)
                at_key = lax.broadcasted_iota(jnp.int32, (rows, size), 1)
                s = jnp.where(jnp.concatenate([at_key <= at_row] * count, axis=0), s, -jnp.inf)
            wide = jnp.broadcast_to(jnp.max(s, axis=1, keepdims=True), (tall, W))
            if not first:
                old = top[head].reshape(tall, W)
                wide = jnp.maximum(old, wide)
            s = (s - spread(wide)) * factor
            w = jnp.exp2(s).astype(jnp.bfloat16)
            o = jnp.dot(w, vals, preferred_element_type=jnp.float32)
            if not first:
                fade = jnp.exp2((old - wide) * factor)
                o = o + acc[head].reshape(tall, 2 * W) * jnp.concatenate([fade, fade], axis=1)
            top[head] = wide.reshape(count, rows, W)
            acc[head] = o.reshape(count, rows, 2 * W)

    def finish(g):
        total = squares[...]
        for j in range(per_group):
            head = g * per_group + j
            lanes = pl.ds(pl.multiple_of(head * W, W), W)
            both = acc[head]
            attended = (both[:, :W] / both[:, W:]).astype(jnp.bfloat16).astype(jnp.float32)
            hidden = rbuf[:, lanes].astype(jnp.float32) + attended
            total = total + hidden * hidden
            top[head] = hidden
        squares[...] = total

    def merge(first, end):
        total = squares[...]
        if first == 0:
            stat_copy.wait_recv()
        pad = jnp.zeros((W - stat.shape[0], stat.shape[1]), jnp.float32)
        far = jnp.transpose(jnp.concatenate([stat[...], pad], axis=0))[:rows]
        for j in range(first, end):
            lanes = slice(j * W, (j + 1) * W)
            o_copy(j).wait_recv()
            both = acc[j]
            near = top[j] * factor + jnp.log(both[:, W:]) * math.log2(math.e)
            share = 1.0 / (1.0 + jnp.exp2(near - jnp.broadcast_to(far[:, j : j + 1], (rows, W))))
            mine = both[:, :W] / both[:, W:]
            attended = mine + (obuf[j].astype(jnp.float32) - mine) * share
            attended = attended.astype(jnp.bfloat16).astype(jnp.float32)
            hidden = rbuf[:, lanes].astype(jnp.float32) + attended
            total = total + hidden * hidden
            top[j] = hidden
        squares[...] = total

    def emit():
        lane = lax.broadcasted_iota(jnp.int32, (rows, W), 1)
        far = jnp.zeros((rows, W), jnp.float32)
        for j in range(per_group):
            both = acc[heads + j]
            total = top[heads + j] * factor + jnp.log(both[:, W:]) * math.log2(math.e)
            far = jnp.where(lane == j, total, far)
            obuf[j] = (both[:, :W] / both[:, W:]).astype(jnp.bfloat16)
        pad = jnp.zeros((stat.shape[1] - rows, W), jnp.float32)
        stat[...] = jnp.transpose(jnp.concatenate([far, pad], axis=0))[: stat.shape[0]]

    def send_o():
        stat_copy.start()
        for j in range(per_group):
            o_copy(j).start()

    def helped(b, carry):
        @pl.when(b == plane)
        def _():
            q3_copy.wait_recv()

        @pl.when((b == plane) & ((col == 0) | (b == 0)))
        def _():
            side_copy(0, plane, 1 - col).wait_recv()

        @pl.when((col == 1) & (b < plane) & ((b == 0) | (b == 1)))
        def _():
            side_copy(0, b, 0).wait_recv()

        attend(heads, 0, [2 * b, 2 * b + 1], False)
        return carry

    def diagonal(g, carry):
        @pl.when(jnp.logical_not(is_top & (g == 0)))
        def _():
            lax.fori_loop(0, per_group, lambda j, inner: query_copy(g * per_group + j).wait(), None)

        attend(g * per_group, g, [me], True)
        return carry

    ahead = jnp.where((col == 0) | is_help, 2, 0)
    groups = kv_heads - skip
    pieces = plane * groups

    def relay_piece(i):
        relay(lax.rem(i, groups) + skip, plane - 1 - i // groups)

    lax.fori_loop(0, kv_heads, diagonal, 0)
    r_in.wait()
    g_in.wait()
    lax.fori_loop(0, jnp.minimum(ahead, pieces), lambda i, carry: relay_piece(i), None)

    @pl.when(is_help)
    def _():
        top[pl.ds(heads, per_group)] = jnp.full((per_group, rows, W), -1e30, jnp.float32)
        acc[pl.ds(heads, per_group)] = jnp.zeros((per_group, rows, 2 * W), jnp.float32)

    @pl.when(is_help & (plane == 0))
    def _():
        lax.fori_loop(0, 1, helped, 0)
        emit()
        send_o()

    @pl.when((col == 0) & (plane == 0))
    def _():
        lax.fori_loop(0, kv_heads, lambda g, carry: finish(g), None)

    def paired(i, carry):
        g = lax.rem(i, groups) + skip
        q = plane - 1 - i // groups
        attend(g * per_group, g, [2 * q + col, 2 * q + 1 + col], False)
        return carry

    def step(i, carry):
        g = lax.rem(i, groups) + skip
        q = plane - 1 - i // groups

        @pl.when((i + ahead < pieces) & jnp.logical_not(is_help & (i + ahead == pieces - 1)))
        def _():
            relay_piece(i + ahead)

        there = by_detour(g, q + col, 1 - col)

        @pl.when(there)
        def _():
            half_side(g, q + col).wait_recv()
            detour(q + col).wait_recv()

        had = ((g == 0) & (q == 0) & (plane > 1)) | (use_detour & (g == detour_g) & (q == plane - 2))

        @pl.when(jnp.logical_not((is_help & (col == 1) & had) | there))
        def _():
            side_copy(g, q + col, 1 - col).wait_recv()

        @pl.when(use_detour & is_help & (col == 1) & (q == plane - 1) & (g == detour_g + 1))
        def _():
            side_copy(detour_g, q, 0).wait_recv()
            detour(q).start()

        final = is_help & (q == 0) & (g == 0)
        whole = is_help & (g == kv_heads - 2) & (q >= 1)
        second = is_help & (g == kv_heads - 1) & (q == 1)
        low = jnp.where(whole, q + 1, jnp.where(second, 1, 0))
        many = jnp.where(final, jnp.where(plane == 1, 2, 1), (whole | second).astype(jnp.int32))
        lax.fori_loop(low, low + many, helped, 0)

        @pl.when(final)
        def _():
            emit()
            relay_piece(pieces - 1)
            send_o()

        later = is_help & (q == 1) & (g == kv_heads - 1)
        start = jnp.where(final & (plane > 1), i - 1, i)
        lax.fori_loop(start, jnp.where(later, start, i + 1), paired, 0)

        @pl.when((col == 0) & (q == 0))
        def _():
            finish(g)

        return carry

    lax.fori_loop(0, pieces, step, 0)

    early = per_group - 2

    def last(g, carry):
        q = jnp.where(is_top & (g == 0), plane, 0)

        @pl.when(is_top & (g == kv_heads - 1))
        def _():
            merge(0, early)

        @pl.when(jnp.logical_not(is_help & (g == 0)))
        def _():
            side_copy(g, q, 0).wait_recv()

        attend(g * per_group, g, [2 * q], False)

        @pl.when(jnp.logical_not(is_top & (g == 0)))
        def _():
            finish(g)

        return carry

    @pl.when(col == 1)
    def _():
        lax.fori_loop(0, kv_heads, last, 0)

    @pl.when(is_top & (col == 0))
    def _():
        merge(0, early)

    @pl.when(is_top)
    def _():
        merge(early, per_group)

    mean = jnp.sum(squares[...], axis=1, keepdims=True) / width
    scale = jnp.broadcast_to(lax.rsqrt(mean + norm_eps), (rows, W))
    for head in range(kv_heads * per_group):
        lanes = slice(head * W, (head + 1) * W)
        gain = gain_ref[lanes].reshape(1, W)
        out_ref[0, :, lanes] = (top[head] * scale * gain).astype(jnp.bfloat16)

    def drain_own(g, carry):
        @pl.when(goes_up(g))
        def _():
            up_copy(g, plane).wait_send()

        @pl.when((col == 0) | (is_help & (g == 0)))
        def _():
            side_copy(g, plane, col).wait_send()

        return carry

    lax.fori_loop(0, kv_heads, drain_own, 0)

    def drain(q, carry):
        def one(g, inner):
            @pl.when(goes_up(g))
            def _():
                up_copy(g, q).wait_send()

            @pl.when(by_detour(g, q, col))
            def _():
                half_side(g, q).wait_send()

            @pl.when(jnp.logical_not(by_detour(g, q, col)))
            def _():
                side_copy(g, q, col).wait_send()

            return inner

        return lax.fori_loop(skip, kv_heads, one, carry)

    lax.fori_loop(0, plane, drain, 0)

    @pl.when(is_top)
    def _():
        q3_copy.wait_send()

    @pl.when(is_help)
    def _():
        stat_copy.wait_send()

        @pl.when(use_detour & (col == 1))
        def _():
            detour(plane - 1).wait_send()

        for j in range(per_group):
            o_copy(j).wait_send()


def body(queries, keys, values, residual, norm_gain):
    count = lax.axis_size("seq")
    rows = queries.shape[1]
    width = queries.shape[2]
    kv_heads = keys.shape[2] // HEAD_WIDTH
    heads = width // HEAD_WIDTH
    planes = count // 2
    per_group = heads // kv_heads
    queries, keys, values, residual, norm_gain = (
        pltpu.with_memory_space_constraint(x, pltpu.HBM)
        for x in (queries, keys, values, residual, norm_gain)
    )
    hbm = pl.BlockSpec(memory_space=pltpu.HBM)
    vmem = pl.BlockSpec(memory_space=pltpu.VMEM)
    return pl.pallas_call(
        functools.partial(kernel, planes, rows, kv_heads, per_group),
        out_shape=pltpu.VMEM(queries.shape, jnp.bfloat16),
        in_specs=[hbm] * 5,
        out_specs=vmem,
        scratch_shapes=[
            pltpu.VMEM((width,), jnp.float32),
            pltpu.VMEM((heads + per_group, rows, HEAD_WIDTH), jnp.bfloat16),
            pltpu.VMEM((rows, width), jnp.bfloat16),
            pltpu.VMEM((kv_heads, count, rows, 2 * HEAD_WIDTH), jnp.bfloat16),
            pltpu.VMEM((heads + per_group, rows, HEAD_WIDTH), jnp.float32),
            pltpu.VMEM((heads + per_group, rows, 2 * HEAD_WIDTH), jnp.float32),
            pltpu.VMEM((per_group, rows, HEAD_WIDTH), jnp.bfloat16),
            pltpu.VMEM((-(-per_group // 8) * 8, -(-rows // HEAD_WIDTH) * HEAD_WIDTH), jnp.float32),
            pltpu.VMEM((rows, HEAD_WIDTH), jnp.float32),
            pltpu.SemaphoreType.DMA((heads + 2,)),
            pltpu.SemaphoreType.DMA((kv_heads, 2)),
            pltpu.SemaphoreType.DMA((kv_heads, planes)),
            pltpu.SemaphoreType.DMA((kv_heads, planes)),
            pltpu.SemaphoreType.DMA((kv_heads, planes)),
            pltpu.SemaphoreType.DMA((kv_heads, planes)),
            pltpu.SemaphoreType.DMA,
            pltpu.SemaphoreType.DMA,
            pltpu.SemaphoreType.DMA((per_group + 1,)),
            pltpu.SemaphoreType.DMA((per_group + 1,)),
            pltpu.SemaphoreType.DMA,
            pltpu.SemaphoreType.DMA,
        ],
        compiler_params=pltpu.CompilerParams(
            collective_id=0, has_side_effects=True, vmem_limit_bytes=54500000
        ),
    )(queries, keys, values, residual, norm_gain)


def solution(mesh):
    rows = P(("groups", "vocab", "batch"), "seq", None)
    return jax.shard_map(
        body,
        mesh=mesh,
        in_specs=(rows, rows, rows, rows, P()),
        out_specs=rows,
        check_vma=False,
    )
```

```python
import functools
import math

import jax
import jax.numpy as jnp
from jax import lax
from jax.experimental import pallas as pl
from jax.experimental.pallas import tpu as pltpu
from jax.sharding import PartitionSpec as P

HEAD_WIDTH = 128
norm_eps = 1e-06
MESH = pl.DeviceIdType.MESH


def kernel(
    planes,
    rows,
    kv_heads,
    per_group,
    q_hbm,
    k_hbm,
    v_hbm,
    r_hbm,
    gain_hbm,
    out_ref,
    gain_ref,
    qbuf,
    rbuf,
    kvbuf,
    top,
    acc,
    obuf,
    stat,
    squares,
    local_sem,
    own_sem,
    up_send,
    up_recv,
    side_send,
    side_recv,
    q3_send,
    q3_recv,
    o_send,
    o_recv,
    x_send,
    x_recv,
):
    W = HEAD_WIDTH
    heads = kv_heads * per_group
    width = heads * W
    me = lax.axis_index("seq")
    plane = me // 2
    col = lax.rem(me, 2)
    above = me + 2
    below = me - 2
    side = me + 1 - 2 * col
    has_up = plane + 1 < planes
    has_down = plane > 0
    is_top = (plane == planes - 1) & (planes > 1)
    is_help = plane == planes - 2
    skip = is_top.astype(jnp.int32)
    factor = math.log2(math.e) / math.sqrt(W)

    barrier = pltpu.get_barrier_semaphore()

    @pl.when(has_down)
    def _():
        pl.semaphore_signal(barrier, inc=1, device_id={"seq": below}, device_id_type=MESH)

    pl.semaphore_signal(barrier, inc=1, device_id={"seq": side}, device_id_type=MESH)

    @pl.when(has_up)
    def _():
        pl.semaphore_signal(barrier, inc=1, device_id={"seq": above}, device_id_type=MESH)

    own = []
    for g in range(kv_heads):
        lanes = slice(g * W, (g + 1) * W)
        pair = (
            pltpu.make_async_copy(k_hbm.at[0, :, lanes], kvbuf.at[g, me, :, :W], own_sem.at[g, 0]),
            pltpu.make_async_copy(v_hbm.at[0, :, lanes], kvbuf.at[g, me, :, W:], own_sem.at[g, 1]),
        )
        for copy in pair:
            copy.start()
        own.append(pair)

    def query_copy(head):
        lanes = pl.ds(pl.multiple_of(head * W, W), W)
        return pltpu.make_async_copy(
            q_hbm.at[0, :, lanes], qbuf.at[head], local_sem.at[head]
        )

    r_in = pltpu.make_async_copy(r_hbm.at[0], rbuf, local_sem.at[heads])
    lax.fori_loop(0, heads, lambda head, carry: query_copy(head).start(), None)
    g_in = pltpu.make_async_copy(gain_hbm, gain_ref, local_sem.at[heads + 1])
    r_in.start()
    g_in.start()

    pl.semaphore_wait(barrier, 1 + has_up.astype(jnp.int32) + has_down.astype(jnp.int32))

    def remote(slot, send_sem, recv_sem, target):
        return pltpu.make_async_remote_copy(
            src_ref=slot,
            dst_ref=slot,
            send_sem=send_sem,
            recv_sem=recv_sem,
            device_id={"seq": target},
            device_id_type=MESH,
        )

    def up_copy(g, q):
        return remote(kvbuf.at[g, 2 * q + col], up_send.at[g, q], up_recv.at[g, q], above)

    def side_copy(g, q, column):
        return remote(kvbuf.at[g, 2 * q + column], side_send.at[g, q], side_recv.at[g, q], side)

    half = rows // 2
    use_detour = planes > 3
    detour_g = 1

    def half_side(g, q):
        slot = kvbuf.at[g, 2 * q, pl.ds(0, half)]
        return remote(slot, side_send.at[g, q], side_recv.at[g, q], side)

    def detour(q):
        slot = kvbuf.at[detour_g, 2 * q, pl.ds(half, half)]
        return remote(slot, x_send, x_recv, above)

    def by_detour(g, q, column):
        return use_detour & is_top & (q == plane - 2) & (g == detour_g) & (column == 0)

    q3_copy = pltpu.make_async_remote_copy(
        src_ref=qbuf.at[pl.ds(0, per_group)],
        dst_ref=qbuf.at[pl.ds(heads, per_group)],
        send_sem=q3_send,
        recv_sem=q3_recv,
        device_id={"seq": below},
        device_id_type=MESH,
    )

    def o_copy(j):
        return remote(obuf.at[j], o_send.at[j], o_recv.at[j], above)

    stat_copy = remote(stat, o_send.at[per_group], o_recv.at[per_group], above)

    def goes_up(g):
        return has_up & jnp.logical_not(is_help & (g == 0))

    for g in range(kv_heads):
        for copy in own[g]:
            copy.wait()

        @pl.when(goes_up(g))
        def _(g=g):
            up_copy(g, plane).start()

        late = is_help & has_down if g >= 2 else False

        @pl.when((col == 0) & jnp.logical_not(late))
        def _(g=g):
            side_copy(g, plane, col).start()

        if g == 0:

            @pl.when((col == 1) & is_help)
            def _():
                side_copy(0, plane, col).start()

    @pl.when(is_top)
    def _():
        lax.fori_loop(0, per_group, lambda j, inner: query_copy(j).wait(), None)
        q3_copy.start()

    squares[...] = jnp.zeros_like(squares)

    def relay(g, q):
        up_copy(g, q).wait_recv()

        @pl.when(goes_up(g))
        def _():
            up_copy(g, q).start()

        paced = is_help & (col == 0)

        @pl.when(by_detour(g, q, col))
        def _():
            half_side(g, q).start()

        @pl.when(jnp.logical_not((paced & (g >= 2) & (q >= 1)) | by_detour(g, q, col)))
        def _():
            side_copy(g, q, col).start()

        @pl.when(paced & (g < 2) & (q == plane - 1))
        def _():
            side_copy(g + 2, plane, col).start()

        @pl.when(paced & (g == 0) & (q < plane - 1))
        def _():
            for h in range(2, kv_heads):
                side_copy(h, q + 1, col).start()

    def attend(base, g, blocks, first):
        keys = jnp.concatenate([kvbuf[g, b, :, :W] for b in blocks], axis=0)
        vals = jnp.concatenate([kvbuf[g, b, :, W:] for b in blocks], axis=0)
        vals = jnp.concatenate([vals, jnp.ones_like(vals)], axis=1)
        size = len(blocks) * rows

        packs = [(at, min(3, per_group - at)) for at in range(0, per_group, 3)]

        def scores(k):
            at, count = packs[k]
            return lax.dot_general(
                qbuf[pl.ds(base + at, count)].reshape(count * rows, W),
                keys,
                (((1,), (1,)), ((), ())),
                preferred_element_type=jnp.float32,
            )

        def spread(x):
            tail = [x[:, : size % W]] if size % W else []
            return jnp.concatenate([x] * (size // W) + tail, axis=1)

        s_next = scores(0)
        for k, (at, count) in enumerate(packs):
            head = pl.ds(base + at, count)
            tall = count * rows
            s = s_next
            if k + 1 < len(packs):
                s_next = scores(k + 1)
            if first:
                at_row = lax.broadcasted_iota(jnp.int32, (rows, size), 0)
                at_key = lax.broadcasted_iota(jnp.int32, (rows, size), 1)
                s = jnp.where(jnp.concatenate([at_key <= at_row] * count, axis=0), s, -jnp.inf)
            wide = jnp.broadcast_to(jnp.max(s, axis=1, keepdims=True), (tall, W))
            if not first:
                old = top[head].reshape(tall, W)
                wide = jnp.maximum(old, wide)
            s = (s - spread(wide)) * factor
            w = jnp.exp2(s).astype(jnp.bfloat16)
            o = jnp.dot(w, vals, preferred_element_type=jnp.float32)
            if not first:
                fade = jnp.exp2((old - wide) * factor)
                o = o + acc[head].reshape(tall, 2 * W) * jnp.concatenate([fade, fade], axis=1)
            top[head] = wide.reshape(count, rows, W)
            acc[head] = o.reshape(count, rows, 2 * W)

    def finish(g):
        total = squares[...]
        for j in range(per_group):
            head = g * per_group + j
            lanes = pl.ds(pl.multiple_of(head * W, W), W)
            both = acc[head]
            attended = (both[:, :W] / both[:, W:]).astype(jnp.bfloat16).astype(jnp.float32)
            hidden = rbuf[:, lanes].astype(jnp.float32) + attended
            total = total + hidden * hidden
            top[head] = hidden * gain_ref[lanes].reshape(1, W)
        squares[...] = total

    def merge(first, end):
        total = squares[...]
        if first == 0:
            stat_copy.wait_recv()
        pad = jnp.zeros((W - stat.shape[0], stat.shape[1]), jnp.float32)
        far = jnp.transpose(jnp.concatenate([stat[...], pad], axis=0))[:rows]
        for j in range(first, end):
            lanes = slice(j * W, (j + 1) * W)
            o_copy(j).wait_recv()
            both = acc[j]
            near = top[j] * factor + jnp.log(both[:, W:]) * math.log2(math.e)
            share = 1.0 / (1.0 + jnp.exp2(near - jnp.broadcast_to(far[:, j : j + 1], (rows, W))))
            mine = both[:, :W] / both[:, W:]
            attended = mine + (obuf[j].astype(jnp.float32) - mine) * share
            attended = attended.astype(jnp.bfloat16).astype(jnp.float32)
            hidden = rbuf[:, lanes].astype(jnp.float32) + attended
            total = total + hidden * hidden
            top[j] = hidden * gain_ref[lanes].reshape(1, W)
        squares[...] = total

    def emit():
        lane = lax.broadcasted_iota(jnp.int32, (rows, W), 1)
        far = jnp.zeros((rows, W), jnp.float32)
        for j in range(per_group):
            both = acc[heads + j]
            total = top[heads + j] * factor + jnp.log(both[:, W:]) * math.log2(math.e)
            far = jnp.where(lane == j, total, far)
            obuf[j] = (both[:, :W] / both[:, W:]).astype(jnp.bfloat16)
        pad = jnp.zeros((stat.shape[1] - rows, W), jnp.float32)
        stat[...] = jnp.transpose(jnp.concatenate([far, pad], axis=0))[: stat.shape[0]]

    def send_o():
        stat_copy.start()
        for j in range(per_group):
            o_copy(j).start()

    def helped(b, carry):
        @pl.when(b == plane)
        def _():
            q3_copy.wait_recv()

        @pl.when((b == plane) & ((col == 0) | (b == 0)))
        def _():
            side_copy(0, plane, 1 - col).wait_recv()

        @pl.when((col == 1) & (b < plane) & ((b == 0) | (b == 1)))
        def _():
            side_copy(0, b, 0).wait_recv()

        attend(heads, 0, [2 * b, 2 * b + 1], False)
        return carry

    def diagonal(g, carry):
        @pl.when(jnp.logical_not(is_top & (g == 0)))
        def _():
            lax.fori_loop(0, per_group, lambda j, inner: query_copy(g * per_group + j).wait(), None)

        attend(g * per_group, g, [me], True)
        return carry

    ahead = jnp.where((col == 0) | is_help, 2, 0)
    groups = kv_heads - skip
    pieces = plane * groups

    def relay_piece(i):
        relay(lax.rem(i, groups) + skip, plane - 1 - i // groups)

    lax.fori_loop(0, kv_heads, diagonal, 0)
    r_in.wait()
    g_in.wait()
    lax.fori_loop(0, jnp.minimum(ahead, pieces), lambda i, carry: relay_piece(i), None)

    @pl.when(is_help)
    def _():
        top[pl.ds(heads, per_group)] = jnp.full((per_group, rows, W), -1e30, jnp.float32)
        acc[pl.ds(heads, per_group)] = jnp.zeros((per_group, rows, 2 * W), jnp.float32)

    @pl.when(is_help & (plane == 0))
    def _():
        lax.fori_loop(0, 1, helped, 0)
        emit()
        send_o()

    @pl.when((col == 0) & (plane == 0))
    def _():
        lax.fori_loop(0, kv_heads, lambda g, carry: finish(g), None)

    def paired(i, carry):
        g = lax.rem(i, groups) + skip
        q = plane - 1 - i // groups
        attend(g * per_group, g, [2 * q + col, 2 * q + 1 + col], False)
        return carry

    def step(i, carry):
        g = lax.rem(i, groups) + skip
        q = plane - 1 - i // groups

        @pl.when((i + ahead < pieces) & jnp.logical_not(is_help & (i + ahead == pieces - 1)))
        def _():
            relay_piece(i + ahead)

        there = by_detour(g, q + col, 1 - col)

        @pl.when(there)
        def _():
            half_side(g, q + col).wait_recv()
            detour(q + col).wait_recv()

        had = ((g == 0) & (q == 0) & (plane > 1)) | (use_detour & (g == detour_g) & (q == plane - 2))

        @pl.when(jnp.logical_not((is_help & (col == 1) & had) | there))
        def _():
            side_copy(g, q + col, 1 - col).wait_recv()

        @pl.when(use_detour & is_help & (col == 1) & (q == plane - 1) & (g == detour_g + 1))
        def _():
            side_copy(detour_g, q, 0).wait_recv()
            detour(q).start()

        final = is_help & (q == 0) & (g == 0)
        whole = is_help & (g == kv_heads - 2) & (q >= 1)
        second = is_help & (g == kv_heads - 1) & (q == 1)
        low = jnp.where(whole, q + 1, jnp.where(second, 1, 0))
        many = jnp.where(final, jnp.where(plane == 1, 2, 1), (whole | second).astype(jnp.int32))
        lax.fori_loop(low, low + many, helped, 0)

        @pl.when(final)
        def _():
            emit()
            relay_piece(pieces - 1)
            send_o()

        later = is_help & (q == 1) & (g == kv_heads - 1)
        start = jnp.where(final & (plane > 1), i - 1, i)
        lax.fori_loop(start, jnp.where(later, start, i + 1), paired, 0)

        @pl.when((col == 0) & (q == 0))
        def _():
            finish(g)

        return carry

    lax.fori_loop(0, pieces, step, 0)

    early = per_group - 2

    def last(g, carry):
        q = jnp.where(is_top & (g == 0), plane, 0)

        @pl.when(is_top & (g == kv_heads - 1))
        def _():
            merge(0, early)

        @pl.when(jnp.logical_not(is_help & (g == 0)))
        def _():
            side_copy(g, q, 0).wait_recv()

        attend(g * per_group, g, [2 * q], False)

        @pl.when(jnp.logical_not(is_top & (g == 0)))
        def _():
            finish(g)

        return carry

    @pl.when(col == 1)
    def _():
        lax.fori_loop(0, kv_heads, last, 0)

    @pl.when(is_top & (col == 0))
    def _():
        merge(0, early)

    @pl.when(is_top)
    def _():
        merge(early, per_group)

    mean = jnp.sum(squares[...], axis=1, keepdims=True) / width
    scale = jnp.broadcast_to(lax.rsqrt(mean + norm_eps), (rows, W))
    for head in range(kv_heads * per_group):
        lanes = slice(head * W, (head + 1) * W)
        out_ref[0, :, lanes] = (top[head] * scale).astype(jnp.bfloat16)

    def drain_own(g, carry):
        @pl.when(goes_up(g))
        def _():
            up_copy(g, plane).wait_send()

        @pl.when((col == 0) | (is_help & (g == 0)))
        def _():
            side_copy(g, plane, col).wait_send()

        return carry

    lax.fori_loop(0, kv_heads, drain_own, 0)

    def drain(q, carry):
        def one(g, inner):
            @pl.when(goes_up(g))
            def _():
                up_copy(g, q).wait_send()

            @pl.when(by_detour(g, q, col))
            def _():
                half_side(g, q).wait_send()

            @pl.when(jnp.logical_not(by_detour(g, q, col)))
            def _():
                side_copy(g, q, col).wait_send()

            return inner

        return lax.fori_loop(skip, kv_heads, one, carry)

    lax.fori_loop(0, plane, drain, 0)

    @pl.when(is_top)
    def _():
        q3_copy.wait_send()

    @pl.when(is_help)
    def _():
        stat_copy.wait_send()

        @pl.when(use_detour & (col == 1))
        def _():
            detour(plane - 1).wait_send()

        for j in range(per_group):
            o_copy(j).wait_send()


def body(queries, keys, values, residual, norm_gain):
    count = lax.axis_size("seq")
    rows = queries.shape[1]
    width = queries.shape[2]
    kv_heads = keys.shape[2] // HEAD_WIDTH
    heads = width // HEAD_WIDTH
    planes = count // 2
    per_group = heads // kv_heads
    queries, keys, values, residual, norm_gain = (
        pltpu.with_memory_space_constraint(x, pltpu.HBM)
        for x in (queries, keys, values, residual, norm_gain)
    )
    hbm = pl.BlockSpec(memory_space=pltpu.HBM)
    vmem = pl.BlockSpec(memory_space=pltpu.VMEM)
    return pl.pallas_call(
        functools.partial(kernel, planes, rows, kv_heads, per_group),
        out_shape=pltpu.VMEM(queries.shape, jnp.bfloat16),
        in_specs=[hbm] * 5,
        out_specs=vmem,
        scratch_shapes=[
            pltpu.VMEM((width,), jnp.float32),
            pltpu.VMEM((heads + per_group, rows, HEAD_WIDTH), jnp.bfloat16),
            pltpu.VMEM((rows, width), jnp.bfloat16),
            pltpu.VMEM((kv_heads, count, rows, 2 * HEAD_WIDTH), jnp.bfloat16),
            pltpu.VMEM((heads + per_group, rows, HEAD_WIDTH), jnp.float32),
            pltpu.VMEM((heads + per_group, rows, 2 * HEAD_WIDTH), jnp.float32),
            pltpu.VMEM((per_group, rows, HEAD_WIDTH), jnp.bfloat16),
            pltpu.VMEM((-(-per_group // 8) * 8, -(-rows // HEAD_WIDTH) * HEAD_WIDTH), jnp.float32),
            pltpu.VMEM((rows, HEAD_WIDTH), jnp.float32),
            pltpu.SemaphoreType.DMA((heads + 2,)),
            pltpu.SemaphoreType.DMA((kv_heads, 2)),
            pltpu.SemaphoreType.DMA((kv_heads, planes)),
            pltpu.SemaphoreType.DMA((kv_heads, planes)),
            pltpu.SemaphoreType.DMA((kv_heads, planes)),
            pltpu.SemaphoreType.DMA((kv_heads, planes)),
            pltpu.SemaphoreType.DMA,
            pltpu.SemaphoreType.DMA,
            pltpu.SemaphoreType.DMA((per_group + 1,)),
            pltpu.SemaphoreType.DMA((per_group + 1,)),
            pltpu.SemaphoreType.DMA,
            pltpu.SemaphoreType.DMA,
        ],
        compiler_params=pltpu.CompilerParams(
            collective_id=0, has_side_effects=True, vmem_limit_bytes=54500000
        ),
    )(queries, keys, values, residual, norm_gain)


def solution(mesh):
    rows = P(("groups", "vocab", "batch"), "seq", None)
    return jax.shard_map(
        body,
        mesh=mesh,
        in_specs=(rows, rows, rows, rows, P()),
        out_specs=rows,
        check_vma=False,
    )
```
